32 devices in a mesh: dp: 4 (over x, y), sp: 8 (over z, core).
Axes of the slice: x: 2, y: 2, z: 4, core: 2. Of those that a mesh axis runs over, the one named last changes fastest.
Arguments:
- x: bfloat16 [8192, 6656], P(('dp', 'sp')), parts along dimension 0
- gain: bfloat16 [6656], replicated
- wq: bfloat16 [6656, 6656], replicated
- wk: bfloat16 [6656, 6656], replicated
- wv: bfloat16 [6656, 6656], replicated
- wo: bfloat16 [6656, 6656], replicated
Outputs:
- output: bfloat16 [8192, 6656], P(('dp', 'sp')), parts along dimension 0
There are 4 independent parts. The reference program is written for one: setup_inputs(seed, part) draws one part's arguments, and reference() takes and returns one part's arrays. A program takes and returns all parts, laid end to end along the dimension named above; an argument that names none is the same for every part.
All inputs are finite; a program needn't handle non-finite values.
Results may differ from the reference program's by a relative error of at most 0.012.
Values are sent between devices in bfloat16 or wider.
A program may use at most 2 GiB of HBM per device.

```python
import jax
import jax.numpy as jnp
from jax import lax

ROWS = 2048
D = 6656
HEADS = 52
KV_HEADS = 52
HEAD = 128
THETA = 10000


def setup_inputs(seed: int = 0, part: int = 0) -> dict:
    kx, kn, kq, kk, kv, ko = jax.random.split(jax.random.key(seed), 6)

    def weights(key, rows, columns):
        return jax.random.normal(key, (rows, columns), jnp.float32) * rows**-0.5

    drawn = {
        "x": jax.random.normal(jax.random.fold_in(kx, part), (ROWS, D), jnp.float32),
        "gain": 1 + 0.1 * jax.random.normal(kn, (D,), jnp.float32),
        "wq": 2 * weights(kq, D, HEADS * HEAD),
        "wk": 2 * weights(kk, D, KV_HEADS * HEAD),
        "wv": 4 * weights(kv, D, KV_HEADS * HEAD),
        "wo": weights(ko, HEADS * HEAD, D),
    }
    return {k: v.astype(jnp.bfloat16) for k, v in drawn.items()}


def normed(x, gain):
    wide = x.astype(jnp.float32)
    scale = lax.rsqrt(jnp.mean(wide * wide, -1, keepdims=True) + 1e-6)
    return (wide * scale * gain.astype(jnp.float32)).astype(jnp.bfloat16)


def turned(t, place, theta):
    half = t.shape[-1] // 2
    angle = place.astype(jnp.float32)[:, None] * theta ** (-jnp.arange(half, dtype=jnp.float32) / half)
    cos, sin = jnp.cos(angle)[:, None], jnp.sin(angle)[:, None]
    a, b = t[..., :half].astype(jnp.float32), t[..., half:].astype(jnp.float32)
    return jnp.concatenate([a * cos - b * sin, b * cos + a * sin], -1).astype(jnp.bfloat16)


def matmul(a, w):
    return jnp.dot(a, w, preferred_element_type=jnp.float32).astype(jnp.bfloat16)


def einsum(form, a, b):
    return jnp.einsum(form, a.astype(jnp.float32), b.astype(jnp.float32))


def attention(q, k, v):
    scores = einsum("tgsd,ugd->gstu", q, k) * q.shape[-1] ** -0.5
    token = jnp.arange(q.shape[0])
    scores = jnp.where(token[:, None] >= token, scores, -jnp.inf)
    weights = jax.nn.softmax(scores, -1).astype(jnp.bfloat16)
    return einsum("gstu,ugd->tgsd", weights, v).astype(jnp.bfloat16)


def reference(x, gain, wq, wk, wv, wo):
    a, place = normed(x, gain), jnp.arange(ROWS)
    q = turned(matmul(a, wq).reshape(ROWS, HEADS, HEAD), place, THETA).reshape(ROWS, KV_HEADS, -1, HEAD)
    k = turned(matmul(a, wk).reshape(ROWS, KV_HEADS, HEAD), place, THETA)
    v = matmul(a, wv).reshape(ROWS, KV_HEADS, HEAD)
    seen = attention(q, k, v).reshape(ROWS, HEADS * HEAD)
    return (x.astype(jnp.float32) + jnp.dot(seen, wo, preferred_element_type=jnp.float32)).astype(jnp.bfloat16)
```

```python
import functools

import jax
import jax.numpy as jnp
from jax import lax
from jax.experimental import pallas as pl
from jax.experimental.pallas import tpu as pltpu
from jax.sharding import PartitionSpec as P

HEAD = 128
THETA = 10000
NEG = -1e30
HIDDEN = 2 * NEG
LOG2E = 1.4426950408889634
VMEM = 60 * 2**20
CHUNKS = (4, 6, 6, 6, 4)
LATE = 1
TILE = 256
WIDE = 512


def normed(x, gain):
    wide = x.astype(jnp.float32)
    scale = lax.rsqrt(jnp.mean(wide * wide, -1, keepdims=True) + 1e-6)
    return (wide * scale * gain.astype(jnp.float32)).astype(jnp.bfloat16)


def _dot(a, b, ca, cb):
    return lax.dot_general(a, b, (((ca,), (cb,)), ((), ())), preferred_element_type=jnp.float32)


def _project(at_ref, own_ref, other_ref, cos_ref, sin_ref, wq_ref, wk_ref, wv_ref, q_ref, kv_ref, a_s, w_s, a_sem, w_sem, *, n):
    j = pl.program_id(0)
    rows = own_ref.shape[0]

    def load(step, slot):
        at = pl.multiple_of(at_ref[0] + lax.rem(step, n) * TILE, TILE)
        kind = lax.div(step, n)
        for i, ref in enumerate((wq_ref, wk_ref, wv_ref)):
            @pl.when(kind == i)
            def _():
                pltpu.make_async_copy(ref.at[:, pl.ds(at, TILE)], w_s.at[slot], w_sem.at[slot]).start()

    slots = w_s.shape[0]

    @pl.when(j == 0)
    def _():
        first = pltpu.make_async_copy(own_ref, a_s.at[pl.ds(0, rows)], a_sem.at[0])
        second = pltpu.make_async_copy(other_ref, a_s.at[pl.ds(rows, rows)], a_sem.at[1])
        first.start()
        load(0, 0)
        second.start()
        for s in range(1, slots - 1):
            load(s, s)
        first.wait()
        second.wait()

    ahead = j + slots - 1

    @pl.when(ahead < 3 * n)
    def _():
        load(ahead, lax.rem(ahead, slots))

    slot = lax.rem(j, slots)
    pltpu.make_async_copy(wq_ref.at[:, pl.ds(0, TILE)], w_s.at[slot], w_sem.at[slot]).wait()
    t = _dot(a_s[...], w_s[slot], 1, 0).astype(jnp.bfloat16)

    def turn(one):
        wide = one.astype(jnp.float32)
        return (wide * cos_ref[...] + pltpu.roll(wide, HEAD // 2, 1) * sin_ref[...]).astype(jnp.bfloat16)

    @pl.when(j < n)
    def _():
        for i in range(2):
            q_ref[i] = turn(t[:, i * HEAD : (i + 1) * HEAD])

    @pl.when((j >= n) & (j < 2 * n))
    def _():
        for i in range(2):
            kv_ref[i] = turn(t[:, i * HEAD : (i + 1) * HEAD])

    @pl.when(j >= 2 * n)
    def _():
        for i in range(2):
            kv_ref[i] = t[:, i * HEAD : (i + 1) * HEAD]


def project(at, own, other, cos, sin, wq, wk, wv, heads):
    n = heads // 2
    rows, d = own.shape
    anywhere = pl.BlockSpec(memory_space=pl.ANY)
    table = pl.BlockSpec((2 * rows, HEAD), lambda j, _: (0, 0))
    return pl.pallas_call(
        functools.partial(_project, n=n),
        grid_spec=pltpu.PrefetchScalarGridSpec(
            num_scalar_prefetch=1,
            grid=(3 * n,),
            in_specs=[anywhere, anywhere, table, table, anywhere, anywhere, anywhere],
            out_specs=[
                pl.BlockSpec((2, 2 * rows, HEAD), lambda j, _: (jnp.minimum(j, n - 1), 0, 0)),
                pl.BlockSpec((2, 2 * rows, HEAD), lambda j, _: (jnp.maximum(j - n, 0), 0, 0)),
            ],
            scratch_shapes=[
                pltpu.VMEM((2 * rows, d), jnp.bfloat16),
                pltpu.VMEM((3, d, TILE), jnp.bfloat16),
                pltpu.SemaphoreType.DMA((2,)),
                pltpu.SemaphoreType.DMA((3,)),
            ],
        ),
        out_shape=[
            jax.ShapeDtypeStruct((heads, 2 * rows, HEAD), jnp.bfloat16),
            jax.ShapeDtypeStruct((2 * heads, 2 * rows, HEAD), jnp.bfloat16),
        ],
        compiler_params=pltpu.CompilerParams(dimension_semantics=("arbitrary",), vmem_limit_bytes=VMEM),
        cost_estimate=pl.CostEstimate(flops=2 * 2 * rows * d * 3 * heads * HEAD, transcendentals=0,
                                      bytes_accessed=3 * heads * HEAD * 2 * (d + 2 * rows) + 4 * rows * d),
        name="project",
    )(at, own, other, cos, sin, wq, wk, wv)


def _part(q, keys, values, masks, e):
    scores = [_dot(k, q, 1, 1) for k in keys]
    scores = [s if m is None else jnp.where(m, s, HIDDEN) for s, m in zip(scores, masks)]
    top = functools.reduce(jnp.maximum, [s.max(axis=0, keepdims=True) for s in scores])
    ones = jnp.ones((8, keys[0].shape[0]), jnp.bfloat16)
    acc = 0.0
    for s, v in zip(scores, values):
        p = jnp.exp2((s - top) * e).astype(jnp.bfloat16)
        acc = acc + _dot(jnp.concatenate([v.T, ones], axis=0), p, 1, 0)
    total = acc[HEAD : HEAD + 1]
    return (acc[:HEAD] * (1 / total)).T, top * e + jnp.log2(total)


def _attention(at_ref, q0_ref, q1_ref, q2_ref, k_ref, v_ref, km_ref, vm_ref, o0_ref, l0_ref, o1_ref, l1_ref, o2_ref, l2_ref, *, e):
    z, core = at_ref[0], at_ref[1]
    rows = q0_ref.shape[1]
    half = rows // 2

    def place(axis):
        i = lax.broadcasted_iota(jnp.int32, (rows, rows), axis) + core * half
        return jnp.where(i >= rows, i - rows, i)

    seen = place(0) <= place(1)
    k, v = k_ref[0], v_ref[0]

    def put(o_ref, l_ref, got):
        o_ref[0] = got[0].astype(o_ref.dtype)
        l_ref[0] = got[1]

    @pl.when(z == 1)
    def _():
        km, vm = km_ref[0], vm_ref[0]
        put(o0_ref, l0_ref, _part(q0_ref[0], [km, k], [vm, v], [None, seen], e))
        put(o1_ref, l1_ref, _part(q1_ref[0], [km, k], [vm, v], [None, None], e))
        put(o2_ref, l2_ref, _part(q2_ref[0], [km, k], [vm, v], [None, None], e))

    @pl.when(z == 2)
    def _():
        put(o0_ref, l0_ref, _part(q0_ref[0], [k], [v], [seen], e))
        put(o1_ref, l1_ref, _part(q1_ref[0], [k], [v], [None], e))

    @pl.when((z == 0) | (z == 3))
    def _():
        put(o0_ref, l0_ref, _part(q0_ref[0], [k], [v], [seen], e))


def attention(at, q0, q1, q2, kv, kvm):
    heads, rows, _ = q0.shape
    block = pl.BlockSpec((1, rows, HEAD), lambda i, _: (i, 0, 0))
    values = pl.BlockSpec((1, rows, HEAD), lambda i, _: (i + heads, 0, 0))
    stats = pl.BlockSpec((1, 1, rows), lambda i, _: (i, 0, 0))
    out = lambda dtype: jax.ShapeDtypeStruct((heads, rows, HEAD), dtype)
    stat = jax.ShapeDtypeStruct((heads, 1, rows), jnp.float32)
    return pl.pallas_call(
        functools.partial(_attention, e=HEAD**-0.5 * LOG2E),
        grid_spec=pltpu.PrefetchScalarGridSpec(
            num_scalar_prefetch=1,
            grid=(heads,),
            in_specs=[block, block, block, block, values, block, values],
            out_specs=[block, stats] * 3,
        ),
        out_shape=[out(jnp.float32), stat, out(jnp.bfloat16), stat, out(jnp.bfloat16), stat],
        compiler_params=pltpu.CompilerParams(dimension_semantics=("arbitrary",), vmem_limit_bytes=VMEM),
        cost_estimate=pl.CostEstimate(flops=heads * 6 * rows * rows * HEAD * 8, transcendentals=heads * 6 * rows * rows,
                                      bytes_accessed=heads * rows * HEAD * 2 * 12),
        name="attention",
    )(at, q0, q1, q2, kv, kv, kvm, kvm)


def _join(at_ref, o0_ref, l0_ref, o1_ref, l1_ref, o2_ref, l2_ref, keep_ref, send_ref):
    z = at_ref[0]
    half = keep_ref.shape[1]
    l0 = l0_ref[0]
    l1 = jnp.where(z >= 2, l1_ref[0], NEG)
    l2 = jnp.where(z == 3, l2_ref[0], NEG)
    top = jnp.maximum(jnp.maximum(l0, l1), l2)
    w = [jnp.exp2(l - top) for l in (l0, l1, l2)]
    total = w[0] + w[1] + w[2]
    w = [jnp.broadcast_to(x / total, (HEAD, 2 * half)).T for x in w]
    out = o0_ref[0] * w[0]
    out += jnp.where(z >= 2, o1_ref[0].astype(jnp.float32), 0.0) * w[1]
    out += jnp.where(z == 3, o2_ref[0].astype(jnp.float32), 0.0) * w[2]
    out = out.astype(jnp.bfloat16)
    keep_ref[0] = out[:half]
    send_ref[0] = out[half:]


def join(at, parts):
    heads, rows, _ = parts[0].shape
    block = pl.BlockSpec((1, rows, HEAD), lambda i, _: (i, 0, 0))
    stats = pl.BlockSpec((1, 1, rows), lambda i, _: (i, 0, 0))
    half = pl.BlockSpec((1, rows // 2, HEAD), lambda i, _: (i, 0, 0))
    out = jax.ShapeDtypeStruct((heads, rows // 2, HEAD), jnp.bfloat16)
    return pl.pallas_call(
        _join,
        grid_spec=pltpu.PrefetchScalarGridSpec(num_scalar_prefetch=1, grid=(heads,), in_specs=[block, stats] * 3, out_specs=[half, half]),
        out_shape=[out, out],
        compiler_params=pltpu.CompilerParams(dimension_semantics=("arbitrary",), vmem_limit_bytes=VMEM),
        cost_estimate=pl.CostEstimate(flops=heads * rows * HEAD * 8, transcendentals=0, bytes_accessed=heads * rows * HEAD * 10),
        name="join",
    )(at, *parts)


def _finish(at_ref, *refs, sizes, first, tiles):
    c = len(sizes)
    keeps, gots, (base_ref, wo_ref, y_ref, a_s, w_s, sem) = refs[:c], refs[c : 2 * c], refs[2 * c :]
    j = pl.program_id(0)
    depth = sum(sizes) * HEAD
    half = wo_ref.shape[0] // 2

    def copies(step, slot):
        got = []
        for i in range(2):
            core = at_ref[1] if i == 0 else 1 - at_ref[1]
            at = pl.multiple_of(core * half + first * HEAD, HEAD)
            got.append(pltpu.make_async_copy(wo_ref.at[pl.ds(at, depth), pl.ds(pl.multiple_of(step * WIDE, WIDE), WIDE)],
                                             w_s.at[slot, pl.ds(i * depth, depth)], sem.at[slot, i]))
        return got

    @pl.when(j == 0)
    def _():
        for copy in copies(0, 0):
            copy.start()
        n = 0
        for ref in (*keeps, *gots):
            for h in range(ref.shape[0]):
                a_s[:, n * HEAD : (n + 1) * HEAD] = ref[h]
                n += 1

    @pl.when(j + 1 < tiles)
    def _():
        for copy in copies(j + 1, lax.rem(j + 1, 2)):
            copy.start()

    slot = lax.rem(j, 2)
    for copy in copies(j, slot):
        copy.wait()
    y_ref[...] = (base_ref[...].astype(jnp.float32) + _dot(a_s[...], w_s[slot], 1, 0)).astype(y_ref.dtype)


def finish(at, keeps, gots, base, wo, first, dtype):
    sizes = [k.shape[0] for k in keeps]
    rows, d = base.shape
    depth = 2 * sum(sizes) * HEAD
    tiles = d // WIDE
    whole = [pl.BlockSpec(t.shape, lambda j, _: (0, 0, 0)) for t in (*keeps, *gots)]
    tile = pl.BlockSpec((rows, WIDE), lambda j, _: (0, j))
    return pl.pallas_call(
        functools.partial(_finish, sizes=sizes, first=first, tiles=tiles),
        grid_spec=pltpu.PrefetchScalarGridSpec(
            num_scalar_prefetch=1,
            grid=(tiles,),
            in_specs=[*whole, tile, pl.BlockSpec(memory_space=pl.ANY)],
            out_specs=tile,
            scratch_shapes=[
                pltpu.VMEM((rows, depth), jnp.bfloat16),
                pltpu.VMEM((2, depth, WIDE), jnp.bfloat16),
                pltpu.SemaphoreType.DMA((2, 2)),
            ],
        ),
        out_shape=jax.ShapeDtypeStruct((rows, d), dtype),
        compiler_params=pltpu.CompilerParams(dimension_semantics=("arbitrary",), vmem_limit_bytes=VMEM),
        cost_estimate=pl.CostEstimate(flops=2 * rows * depth * d, transcendentals=0, bytes_accessed=2 * depth * d + 6 * rows * d),
        name="finish",
    )(at, *keeps, *gots, base, wo)


def solution(mesh):
    size = mesh.shape["sp"]

    def along(t, pairs):
        return lax.ppermute(t, "sp", pairs)

    swap = [(i, i ^ 1) for i in range(size)]
    left1 = [(i, i - 2) for i in range(4, size)]
    left2 = [(i, i - 4) for i in range(6, size)]
    right1 = [(i - 2, i) for i in range(4, size)]
    right2 = [(i - 4, i) for i in range(6, size)]
    states = [(0, 2), (1, 3)]

    def step(x, gain, wq, wk, wv, wo):
        own = x.shape[0]
        sp = lax.axis_index("sp")
        z, core = sp // 2, sp % 2
        at = jnp.stack([z, core]).astype(jnp.int32)
        mine = normed(x, gain)
        other = normed(along(x, swap), gain)

        half = HEAD // 2
        place = z * 2 * own + (jnp.arange(2 * own) + core * own) % (2 * own)
        angle = place.astype(jnp.float32)[:, None] * THETA ** (-jnp.arange(half, dtype=jnp.float32) / half)
        cos, sin = jnp.cos(angle), jnp.sin(angle)
        cos, sin = jnp.concatenate([cos, cos], -1), jnp.concatenate([-sin, sin], -1)

        starts = [sum(CHUNKS[:i]) for i in range(len(CHUNKS))]
        column = core * (wq.shape[1] // 2)
        sent = []
        for first, heads in zip(starts, CHUNKS):
            where = (column + first * HEAD).astype(jnp.int32)[None]
            q, kv = project(where, mine, other, cos, sin, wq, wk, wv, heads)
            sent.append((q, kv, along(q, left1), along(q, left2), along(kv, states)))
        parts = []
        for q, kv, q1, q2, kvm in sent:
            o0, l0, o1, l1, o2, l2 = attention(at, q, q1, q2, kv, kvm)
            parts.append((o0, l0, along(o1, right1), along(l1, right1), along(o2, right2), along(l2, right2)))
        keeps, gots = [], []
        for part in parts:
            keep, send = join(at, part)
            keeps.append(keep)
            gots.append(along(send, swap))
        n = len(CHUNKS) - LATE
        y = finish(at, keeps[:n], gots[:n], x, wo, 0, jnp.float32)
        return finish(at, keeps[n:], gots[n:], y, wo, starts[n], jnp.bfloat16)

    tokens, whole = P(("dp", "sp"), None), P(None, None)
    return jax.shard_map(
        step,
        mesh=mesh,
        in_specs=(tokens, P(None), whole, whole, whole, whole),
        out_specs=tokens,
        check_vma=False,
    )
```
